32 devices in a mesh: rep: 4 (over z), head: 4 (over y, core), pair: 2 (over x).
Axes of the slice: x: 2, y: 2, z: 4, core: 2. Of those that a mesh axis runs over, the one named last changes fastest.
Arguments:
- queries: bfloat16 [96, 8192], P(('rep', 'pair'), 'head'), may hold values from -24 to 24
- new_keys: bfloat16 [96, 1024], P(('rep', 'pair'), 'head'), may hold values from -6 to 6
- new_values: bfloat16 [96, 1024], P(('rep', 'pair'), 'head'), may hold values from -6 to 6
- key_cache: bfloat16 [96, 1024, 1024], P(('rep', 'pair'), None, 'head'), may hold values from -6 to 6
- value_cache: bfloat16 [96, 1024, 1024], P(('rep', 'pair'), None, 'head'), may hold values from -6 to 6
- lengths: int32 [96], P(('rep', 'pair')), may hold values from 2 to 1024
- residual: bfloat16 [96, 8192], P('head', ('rep', 'pair')), may hold values from -36 to 36
- norm_gain: float32 [8192], replicated, may hold values from 0.5 to 1.5
- out_weight: bfloat16 [8192, 8192], P('head', ('rep', 'pair')), may hold values from -0.5 to 0.5
- gate_weight: bfloat16 [8192, 28672], P('head', ('rep', 'pair')), may hold values from -0.0625 to 0.0625
- up_weight: bfloat16 [8192, 28672], P('head', ('rep', 'pair')), may hold values from -0.0625 to 0.0625
- down_weight: bfloat16 [28672, 8192], P(('rep', 'pair'), 'head'), may hold values from -0.03125 to 0.03125
Outputs:
- hidden_state: bfloat16 [96, 8192], P('head', ('rep', 'pair'))
- ffn_out: bfloat16 [96, 8192], P(('rep', 'pair'), 'head')
The draws below stay inside these ranges and needn't reach their ends.
Inputs may be any that keep to these rules, and one draw needn't show every extreme that they name: Cache slots 0 to lengths - 1 of a row are live, the others are ignored.
All inputs are finite; a program needn't handle non-finite values.
Results may differ from the reference program's by a relative error of at most 0.0095.
Values may be sent and summed in bfloat16 or wider, within the bound.
A program may use at most 128 MiB of HBM per device.

```python
import jax
import jax.numpy as jnp
from jax import lax

D = 8192
FF = 28672
HEADS = 64
KV_HEADS = 8
HEAD_DIM = 128
CACHE = 1024
ROWS = 96
Q_WIDTH = 8192
KV_WIDTH = 1024


def drawn_cache_keys(key):
    base_key = jax.random.fold_in(key, 11)
    drawn_keys = jnp.clip(jax.random.normal(base_key, (ROWS, CACHE, KV_WIDTH), jnp.float32), -6.0, 6.0)
    return drawn_keys


def draw_key_cache(key, part):
    return drawn_cache_keys(key).astype(jnp.bfloat16)


def draw_queries(key, part):
    noise_key = jax.random.fold_in(key, 13)
    drawn = jnp.clip(jax.random.normal(noise_key, (ROWS, Q_WIDTH), jnp.float32), -6.0, 6.0)
    return drawn.astype(jnp.bfloat16)


def draw_residual(key, part):
    base_key = jax.random.fold_in(key, 17)
    drawn = jnp.clip(jax.random.normal(base_key, (ROWS, D), jnp.float32), -6.0, 6.0)
    return drawn.astype(jnp.bfloat16)


def place_ends(entries, stream_key, low, high):
    extent = entries.shape
    place = [jax.random.randint(jax.random.fold_in(stream_key, axis), (), 0, extent[axis]) for axis in range(len(extent))]
    entries = entries.at[tuple(place)].set(low)
    longest = extent.index(max(extent))
    place[longest] = (place[longest] + 1) % extent[longest]
    return entries.at[tuple(place)].set(high)


def block_scale(key, shape, shards, low, high):
    def one(dim, shards_of):
        draws = jax.random.uniform(jax.random.fold_in(jax.random.fold_in(key, 6), dim), (shards_of,), jnp.float32, low / len(shards), high / len(shards))
        return jnp.repeat(jnp.exp(draws), shape[dim] // shards_of).reshape((-1,) + (1,) * (len(shape) - dim - 1))

    level = one(*shards[0])
    for cut in shards[1:]:
        level = level * one(*cut)
    return level


def gaussian(key, dims, spread, reach, cuts=(), kind=jnp.bfloat16):
    entries = spread * jax.random.normal(key, dims, jnp.float32)
    if cuts:
        entries = entries * block_scale(key, dims, cuts, -0.22, 0.18)
    return jnp.clip(entries, -reach, reach).astype(kind)


def setup_inputs(seed: int = 0) -> dict:
    key_of = jax.random.split(jax.random.key(seed), 13)
    queries = draw_queries(jax.random.fold_in(key_of[12], 71), 0)
    new_keys = gaussian(key_of[1], (ROWS, KV_WIDTH), 1.0, 6.0, ((0, 8), (1, 4)))
    new_values = gaussian(key_of[2], (ROWS, KV_WIDTH), 1.0, 6.0, ((0, 8), (1, 4)))
    key_cache = draw_key_cache(jax.random.fold_in(key_of[12], 71), 0)
    value_cache = gaussian(key_of[4], (ROWS, CACHE, KV_WIDTH), 1.0, 6.0, ((0, 8), (2, 4)))
    lengths = place_ends(jax.random.randint(key_of[5], (ROWS,), 2, CACHE + 1), jax.random.fold_in(key_of[5], 1), 2, CACHE).astype(jnp.int32)
    residual = draw_residual(jax.random.fold_in(key_of[12], 71), 0)
    norm_gain = jnp.clip(1.0 + 0.1 * jax.random.normal(key_of[7], (D,), jnp.float32), 0.5, 1.5)
    out_weight = gaussian(key_of[8], (Q_WIDTH, D), (Q_WIDTH // 64) ** -0.5, 0.5, ((0, 4), (1, 8)))
    gate_weight = gaussian(key_of[9], (D, FF), D ** -0.5, 0.0625, ((0, 4), (1, 8)))
    up_weight = gaussian(key_of[10], (D, FF), D ** -0.5, 0.0625, ((0, 4), (1, 8)))
    down_weight = gaussian(key_of[11], (FF, D), FF ** -0.5, 0.03125, ((0, 8), (1, 4)))
    return {"queries": queries, "new_keys": new_keys, "new_values": new_values, "key_cache": key_cache, "value_cache": value_cache, "lengths": lengths, "residual": residual, "norm_gain": norm_gain, "out_weight": out_weight, "gate_weight": gate_weight, "up_weight": up_weight, "down_weight": down_weight}


def attend_row(row_item):
    query_row, key_new, value_new, cached_keys, cached_values, length = row_item
    group_size = HEADS // KV_HEADS
    score_scale = HEAD_DIM ** (-0.5)
    query_row = query_row.astype(jnp.float32).reshape(KV_HEADS, group_size, HEAD_DIM)
    cached_keys = cached_keys.astype(jnp.float32).reshape(CACHE, KV_HEADS, HEAD_DIM)
    cached_values = cached_values.astype(jnp.float32).reshape(CACHE, KV_HEADS, HEAD_DIM)
    key_new = key_new.astype(jnp.float32).reshape(KV_HEADS, HEAD_DIM)
    value_new = value_new.astype(jnp.float32).reshape(KV_HEADS, HEAD_DIM)
    scores = jnp.einsum('hgd,chd->hgc', query_row, cached_keys) * score_scale
    live_mask = jnp.arange(CACHE, dtype=jnp.int32) < length
    scores = jnp.where(live_mask[None, None, :], scores, -jnp.inf)
    own_score = jnp.einsum('hgd,hd->hg', query_row, key_new) * score_scale
    row_top = jnp.maximum(lax.optimization_barrier(jnp.max(scores, axis=2)), own_score)
    weights = jnp.exp(scores - row_top[:, :, None])
    own_weight = jnp.exp(own_score - row_top)
    weight_total = lax.optimization_barrier(jnp.sum(weights, axis=2)) + own_weight
    weights = lax.optimization_barrier(weights.astype(jnp.bfloat16)).astype(jnp.float32)
    own_weight = lax.optimization_barrier(own_weight.astype(jnp.bfloat16)).astype(jnp.float32)
    mixture = jnp.einsum('hgc,chd->hgd', weights, cached_values) + own_weight[:, :, None] * value_new[:, None, :]
    return (mixture / weight_total[:, :, None]).astype(jnp.bfloat16).reshape(HEADS * HEAD_DIM)

def reference(queries, new_keys, new_values, key_cache, value_cache, lengths, residual, norm_gain, out_weight, gate_weight, up_weight, down_weight):
    attn = lax.map(attend_row, (queries, new_keys, new_values, key_cache, value_cache, lengths))
    projected = jnp.dot(attn, out_weight, preferred_element_type=jnp.float32)
    hidden_state = (residual.astype(jnp.float32) + projected).astype(jnp.bfloat16)
    state_f = hidden_state.astype(jnp.float32)
    mean_square = lax.optimization_barrier(jnp.mean(state_f * state_f, axis=1, keepdims=True))
    normed = (state_f * lax.rsqrt(mean_square + 1e-05) * norm_gain).astype(jnp.bfloat16)
    gate_full = jnp.dot(normed, gate_weight, preferred_element_type=jnp.float32)
    up_full = jnp.dot(normed, up_weight, preferred_element_type=jnp.float32)
    hidden = (jax.nn.silu(gate_full) * up_full).astype(jnp.bfloat16)
    ffn_out = jnp.dot(hidden, down_weight, preferred_element_type=jnp.float32).astype(jnp.bfloat16)
    return (hidden_state, ffn_out)
```

```python
import functools

import jax
import jax.numpy as jnp
from jax import lax
from jax.experimental import pallas as pl
from jax.experimental.pallas import tpu as pltpu
from jax.sharding import PartitionSpec as P

HEADS = 64
KV_HEADS = 8
HEAD_DIM = 128
CHUNKS = 7
SLOTS = 4
MESH = pl.DeviceIdType.MESH
F32 = jnp.float32
BF16 = jnp.bfloat16


def kernel(
    R, H, PR,
    len_ref, q_ref, nk_ref, nv_ref, res_ref, gain_ref,
    k_hbm, v_hbm, ow_hbm, gw_hbm, uw_hbm, dw_hbm,
    hid_out, ffn_out,
    kbuf, vbuf, ow, gw, uw, dw,
    qs, nk32, nv32, ao, agb, pb, bsend, brecv, hsb, cb, xs, xbf,
    ss_send, ss_recv, rscale, dsend, drecv, eb, hx, acc, fsend, frecv,
    kv_sem, w_sem,
    a_s, a_r, b_s, b_r, c_s, c_r, s_s, s_r, d_s, d_r, e_s, e_r, f_s, f_r,
):
    G = R * PR
    gpb = G // H
    rep = lax.axis_index("rep")
    h = lax.axis_index("head")
    pair = lax.axis_index("pair")
    g = rep * PR + pair
    b = q_ref.shape[0]
    slots = kbuf.shape[1]
    kvl = kbuf.shape[2] // HEAD_DIM
    grp = HEADS // KV_HEADS
    nq = kvl * grp
    rb = hsb.shape[0]
    cb_cols = hsb.shape[1]
    C = gw.shape[2]
    D = gain_ref.shape[1]
    scale = HEAD_DIM ** (-0.5)

    def kcopy(r):
        s = lax.rem(r, SLOTS)
        return pltpu.make_async_copy(k_hbm.at[r], kbuf.at[s], kv_sem.at[0, s])

    def vcopy(r):
        s = lax.rem(r, SLOTS)
        return pltpu.make_async_copy(v_hbm.at[r], vbuf.at[s], kv_sem.at[1, s])

    def ow_copy():
        return pltpu.make_async_copy(ow_hbm, ow, w_sem.at[3, 0])

    def g_copy(c):
        return pltpu.make_async_copy(
            gw_hbm.at[:, pl.ds(pl.multiple_of(c * C, C), C)], gw.at[c], w_sem.at[0, c])

    def u_copy(c):
        return pltpu.make_async_copy(
            uw_hbm.at[:, pl.ds(pl.multiple_of(c * C, C), C)], uw.at[c], w_sem.at[1, c])

    def d_copy(c):
        return pltpu.make_async_copy(
            dw_hbm.at[pl.ds(pl.multiple_of(c * C, C), C), :], dw.at[c], w_sem.at[2, c])

    def to_group(src, dst, ss, rs, gd):
        return pltpu.make_async_remote_copy(
            src_ref=src, dst_ref=dst, send_sem=ss, recv_sem=rs,
            device_id=(gd // PR, h, lax.rem(gd, PR)), device_id_type=MESH)

    def to_head(src, dst, ss, rs, hd):
        return pltpu.make_async_remote_copy(
            src_ref=src, dst_ref=dst, send_sem=ss, recv_sem=rs,
            device_id=(rep, hd, pair), device_id_type=MESH)

    for r in range(min(SLOTS, b)):
        kcopy(r).start()
        vcopy(r).start()
    ow_copy().start()
    for i in range(nq):
        qs[pl.ds(i, b, stride=nq), :] = q_ref[:, i * HEAD_DIM:(i + 1) * HEAD_DIM].astype(F32)
    nk32[...] = nk_ref[...].astype(F32)
    nv32[...] = nv_ref[...].astype(F32)

    def attend(r, _):
        s = lax.rem(r, SLOTS)
        kcopy(r).wait()
        q16 = qs[pl.ds(pl.multiple_of(r * nq, nq), nq), :]
        own_of = lax.broadcasted_iota(jnp.int32, (nq, HEAD_DIM), 0) // grp
        qbd = jnp.concatenate(
            [jnp.where(own_of == j, q16, 0.0) for j in range(kvl)], axis=1) if kvl > 1 else q16
        sc = lax.dot_general(
            qbd.astype(BF16), kbuf[s], (((1,), (1,)), ((), ())), preferred_element_type=F32) * scale
        ids = lax.broadcasted_iota(jnp.int32, (nq, slots), 1)
        sc = jnp.where(ids < len_ref[r], sc, -jnp.inf)
        own = jnp.sum(qbd * nk32[pl.ds(r, 1), :], axis=1, keepdims=True) * scale
        top = jnp.maximum(jnp.max(sc, axis=1, keepdims=True), own)
        w = jnp.exp(sc - top)
        ownw = jnp.exp(own - top)
        tot = jnp.sum(w, axis=1, keepdims=True) + ownw
        vcopy(r).wait()
        o = jnp.dot(w.astype(BF16), vbuf[s], preferred_element_type=F32)
        o = (o + ownw.astype(BF16).astype(F32) * nv32[pl.ds(r, 1), :]) / tot
        for j in range(kvl):
            ao[pl.ds(pl.multiple_of(r * nq + j * grp, grp), grp), :] = (
                o[j * grp:(j + 1) * grp, j * HEAD_DIM:(j + 1) * HEAD_DIM])

        @pl.when(r + SLOTS < b)
        def _():
            kcopy(r + SLOTS).start()
            vcopy(r + SLOTS).start()

        @pl.when(jnp.logical_and(r >= 3, r < 3 + CHUNKS))
        def _():
            g_copy(r - 3).start()
        return 0

    lax.fori_loop(0, b, attend, 0)
    agb[g] = jnp.zeros(agb.shape[1:], BF16)
    for i in range(nq):
        agb[g, 0:b, i * HEAD_DIM:(i + 1) * HEAD_DIM] = ao[pl.ds(i, b, stride=nq), :].astype(BF16)

    def a_copy(d):
        gd = lax.rem(g + d, G)
        return to_group(agb.at[g], agb.at[g], a_s.at[d], a_r.at[g], gd)

    def a_in(d):
        gs = lax.rem(g + d, G)
        return to_group(agb.at[gs], agb.at[gs], a_s.at[d], a_r.at[gs], gs)

    for d in range(1, G):
        a_copy(d).start()
    for c in range(CHUNKS):
        u_copy(c).start()
    for c in range(CHUNKS):
        d_copy(c).start()
    ow_copy().wait()
    for d in range(1, G):
        a_in(d).wait_recv()

    pad = agb.shape[1]
    full = agb[...].reshape(G * pad, agb.shape[2])
    prod = jnp.dot(full, ow[...], preferred_element_type=F32)
    for a in range(G):
        pb[a * b:(a + 1) * b, :] = prod[a * pad:a * pad + b, :]
    for j in range(H):
        bsend[j] = pb[j * rb:(j + 1) * rb, :].astype(BF16)

    def b_copy(d):
        hd = lax.rem(h + d, H)
        return to_head(bsend.at[hd], brecv.at[h], b_s.at[d], b_r.at[h], hd)

    def b_in(d):
        hs = lax.rem(h + d, H)
        return to_head(bsend.at[hs], brecv.at[hs], b_s.at[d], b_r.at[hs], hs)

    for d in range(1, H):
        b_copy(d).start()
    total = res_ref[...].astype(F32) + pb[pl.ds(pl.multiple_of(h * rb, rb), rb), :]
    for d in range(1, H):
        b_in(d).wait_recv()
        total = total + brecv[lax.rem(h + d, H)].astype(F32)
    state = total.astype(BF16)
    hid_out[...] = state
    hsb[...] = state

    hd_c = g // gpb
    slot_c = h * gpb + lax.rem(g, gpb)

    def c_copy(d):
        gd = lax.rem(g + d, G)
        return pltpu.make_async_remote_copy(
            src_ref=hsb, dst_ref=cb.at[slot_c], send_sem=c_s.at[d], recv_sem=c_r.at[slot_c],
            device_id=(gd // PR, hd_c, lax.rem(gd, PR)), device_id_type=MESH)

    for d in range(1, G):
        c_copy(d).start()

    @pl.when(hd_c != h)
    def _():
        c_copy(0).start()

    @pl.when(hd_c == h)
    def _():
        cb[slot_c] = state

    for j in range(H):
        for k in range(gpb):
            mine = jnp.logical_and(h == j, g == h * gpb + k)

            @pl.when(jnp.logical_not(mine))
            def _():
                pltpu.make_async_remote_copy(
                    src_ref=hsb, dst_ref=cb.at[j * gpb + k], send_sem=c_s.at[0],
                    recv_sem=c_r.at[j * gpb + k], device_id=(rep, lax.rem(h + 1, H), pair),
                    device_id_type=MESH).wait_recv()

    for j in range(H):
        sq = jnp.zeros((rb, 1), F32)
        for k in range(gpb):
            xv = cb[j * gpb + k].astype(F32)
            sq = sq + jnp.sum(xv * xv, axis=1, keepdims=True)
            gain = gain_ref[:, pl.ds(pl.multiple_of((h * gpb + k) * cb_cols, cb_cols), cb_cols)]
            xs[j * rb:(j + 1) * rb, k * cb_cols:(k + 1) * cb_cols] = xv * gain
        ss_send[j] = jnp.broadcast_to(sq, (rb, 128))
    xbf[...] = xs[...].astype(BF16)

    def s_copy(d):
        hd = lax.rem(h + d, H)
        return to_head(ss_send.at[hd], ss_recv.at[h], s_s.at[d], s_r.at[h], hd)

    def s_in(d):
        hs = lax.rem(h + d, H)
        return to_head(ss_send.at[hs], ss_recv.at[hs], s_s.at[d], s_r.at[hs], hs)

    for d in range(1, H):
        s_copy(d).start()

    def d_out(c, d):
        hd = lax.rem(h + d, H)
        return to_head(dsend.at[c, hd], drecv.at[c, h], d_s.at[c, d], d_r.at[c, h], hd)

    def d_in(c, d):
        hs = lax.rem(h + d, H)
        return to_head(dsend.at[c, hs], drecv.at[c, hs], d_s.at[c, d], d_r.at[c, hs], hs)

    def e_out(c, d):
        hd = lax.rem(h + d, H)
        return to_head(eb.at[c, h], eb.at[c, h], e_s.at[c, d], e_r.at[c, h], hd)

    def e_in(c, d):
        hs = lax.rem(h + d, H)
        return to_head(eb.at[c, hs], eb.at[c, hs], e_s.at[c, d], e_r.at[c, hs], hs)

    def expand(c):
        for m, (copy, wt) in enumerate(((g_copy, gw), (u_copy, uw))):
            copy(c).wait()
            part = jnp.dot(xbf[...], wt[c], preferred_element_type=F32)
            for j in range(H):
                dsend[c, j, :, m * C:(m + 1) * C] = part[j * rb:(j + 1) * rb, :].astype(BF16)
        for d in range(1, H):
            d_out(c, d).start()

    def activate(c):
        both = dsend[c, h].astype(F32)
        for d in range(1, H):
            d_in(c, d).wait_recv()
            both = both + drecv[c, lax.rem(h + d, H)].astype(F32)
        both = both * rscale[:, 0:1]
        gate = both[:, :C]
        up = both[:, C:]
        eb[c, h] = (gate / (1.0 + jnp.exp(-gate)) * up).astype(BF16)
        for d in range(1, H):
            e_out(c, d).start()

    def contract(c):
        d_copy(c).wait()
        for d in range(1, H):
            e_in(c, d).wait_recv()
        for j in range(H):
            hx[j * rb:(j + 1) * rb, :] = eb[c, j].astype(F32)
        acc[...] += jnp.dot(hx[...].astype(BF16), dw[c], preferred_element_type=F32)

    acc[...] = jnp.zeros_like(acc)
    lag1, lag2 = 2, 4

    def stage(t, _):
        @pl.when(t < CHUNKS)
        def _():
            expand(t)

        @pl.when(t == lag1 - 1)
        def _():
            sq = ss_send[h]
            for d in range(1, H):
                s_in(d).wait_recv()
                sq = sq + ss_recv[lax.rem(h + d, H)]
            rscale[...] = lax.rsqrt(sq * (1.0 / D) + 1e-05)

        @pl.when(jnp.logical_and(t >= lag1, t < CHUNKS + lag1))
        def _():
            activate(t - lag1)

        @pl.when(t >= lag2)
        def _():
            contract(t - lag2)
        return 0

    lax.fori_loop(0, CHUNKS + lag2, stage, 0)

    for a in range(G):
        fsend[a] = acc[a * b:(a + 1) * b, :].astype(BF16)

    def f_copy(d):
        gd = lax.rem(g + d, G)
        return to_group(fsend.at[gd], frecv.at[g], f_s.at[d], f_r.at[g], gd)

    def f_in(d):
        gs = lax.rem(g + d, G)
        return to_group(fsend.at[gs], frecv.at[gs], f_s.at[d], f_r.at[gs], gs)

    for d in range(1, G):
        f_copy(d).start()
    out = fsend[g].astype(F32)
    for d in range(1, G):
        f_in(d).wait_recv()
        out = out + frecv[lax.rem(g + d, G)].astype(F32)
    ffn_out[...] = out.astype(BF16)

    for d in range(1, G):
        a_copy(d).wait_send()
        c_copy(d).wait_send()
        f_copy(d).wait_send()

    @pl.when(hd_c != h)
    def _():
        c_copy(0).wait_send()

    for d in range(1, H):
        b_copy(d).wait_send()
        s_copy(d).wait_send()

    def drain(c, _):
        for d in range(1, H):
            d_out(c, d).wait_send()
            e_out(c, d).wait_send()
        return 0

    lax.fori_loop(0, CHUNKS, drain, 0)


def local(
    R, H, PR,
    queries, new_keys, new_values, key_cache, value_cache, lengths,
    residual, norm_gain, out_weight, gate_weight, up_weight, down_weight,
):
    G = R * PR
    b, qw = queries.shape
    kvw = new_keys.shape[1]
    slots = key_cache.shape[1]
    rb, oc = residual.shape
    D = norm_gain.shape[0]
    fin, units = gate_weight.shape
    dout = down_weight.shape[1]
    C = units // CHUNKS
    B = b * G
    nq = qw // HEAD_DIM
    pad = -(-b // 16) * 16
    gpb = G // H
    V, S = pltpu.VMEM, pltpu.SemaphoreType.DMA
    vm = pl.BlockSpec(memory_space=pltpu.VMEM)
    hb = pl.BlockSpec(memory_space=pl.ANY)
    return pl.pallas_call(
        functools.partial(kernel, R, H, PR),
        out_shape=(
            jax.ShapeDtypeStruct((rb, oc), BF16),
            jax.ShapeDtypeStruct((b, dout), BF16),
        ),
        in_specs=[pl.BlockSpec(memory_space=pltpu.SMEM)] + [vm] * 5 + [hb] * 6,
        out_specs=(vm, vm),
        scratch_shapes=[
            V((SLOTS, slots, kvw), BF16), V((SLOTS, slots, kvw), BF16),
            V(out_weight.shape, BF16),
            V((CHUNKS, fin, C), BF16), V((CHUNKS, fin, C), BF16), V((CHUNKS, C, dout), BF16),
            V((b * nq, HEAD_DIM), F32), V((b, kvw), F32), V((b, kvw), F32),
            V((b * nq, HEAD_DIM), F32), V((G, pad, qw), BF16),
            V((B, oc), F32), V((H, rb, oc), BF16), V((H, rb, oc), BF16),
            V((rb, oc), BF16), V((H * gpb, rb, oc), BF16),
            V((B, fin), F32), V((B, fin), BF16),
            V((H, rb, 128), F32), V((H, rb, 128), F32), V((rb, 128), F32),
            V((CHUNKS, H, rb, 2 * C), BF16), V((CHUNKS, H, rb, 2 * C), BF16),
            V((CHUNKS, H, rb, C), BF16), V((B, C), F32), V((B, dout), F32),
            V((G, b, dout), BF16), V((G, b, dout), BF16),
            S((2, SLOTS)), S((4, CHUNKS)),
            S((G,)), S((G,)), S((H,)), S((H,)), S((G,)), S((H * gpb,)), S((H,)), S((H,)),
            S((CHUNKS, H)), S((CHUNKS, H)), S((CHUNKS, H)), S((CHUNKS, H)), S((G,)), S((G,)),
        ],
        compiler_params=pltpu.CompilerParams(
            has_side_effects=True, vmem_limit_bytes=66_900_000),
        name="decode_step",
    )(
        lengths, queries, new_keys, new_values, residual, norm_gain.reshape(1, D),
        key_cache, value_cache, out_weight, gate_weight, up_weight, down_weight,
    )


def solution(mesh):
    placed = (
        P(("rep", "pair"), "head"),
        P(("rep", "pair"), "head"),
        P(("rep", "pair"), "head"),
        P(("rep", "pair"), None, "head"),
        P(("rep", "pair"), None, "head"),
        P(("rep", "pair")),
        P("head", ("rep", "pair")),
        P(),
        P("head", ("rep", "pair")),
        P("head", ("rep", "pair")),
        P("head", ("rep", "pair")),
        P(("rep", "pair"), "head"),
    )
    return jax.shard_map(
        functools.partial(local, mesh.shape["rep"], mesh.shape["head"], mesh.shape["pair"]),
        mesh=mesh,
        in_specs=placed,
        out_specs=(P("head", ("rep", "pair")), P(("rep", "pair"), "head")),
        check_vma=False,
    )
```
